32 devices in a mesh: ctx: 8 (over y, x, core), tp: 4 (over z).
Axes of the slice: x: 2, y: 2, z: 4, core: 2. Of those that a mesh axis runs over, the one named last changes fastest.
Arguments:
- queries: bfloat16 [2048, 8192], P('ctx', 'tp'), may hold values from -8 to 8
- keys: bfloat16 [2048, 1024], P('ctx'), may hold values from -6 to 6
- values: bfloat16 [2048, 1024], P('ctx'), may hold values from -6 to 6
Outputs:
- attended: bfloat16 [2048, 8192], P('ctx', 'tp')
The draws below stay inside these ranges and needn't reach their ends.
All inputs are finite; a program needn't handle non-finite values.
Results may differ from the reference program's by a relative error of at most 0.0032.
Values may be sent and summed in bfloat16 or wider, within the bound.
A program may use at most 64 MiB of HBM per device.

```python
import jax
import jax.numpy as jnp
from jax import lax

HEADS = 64
KV_HEADS = 8
HEAD_DIM = 128
TOKENS = 2048


def draw_keys(key, part):
    drawn = jnp.clip(jax.random.normal(jax.random.fold_in(key, 11), (TOKENS, KV_HEADS * HEAD_DIM), jnp.float32), -6.0, 6.0)
    return drawn.astype(jnp.bfloat16)


def draw_queries(key, part):
    drawn = jnp.clip(2.5 * jax.random.normal(jax.random.fold_in(key, 13), (TOKENS, HEADS * HEAD_DIM), jnp.float32), -8.0, 8.0)
    return drawn.astype(jnp.bfloat16)


def block_levels(stream_key, dims, pieces, least, high):
    factor_of, own = 1.0, jax.random.fold_in(stream_key, 6)
    for dim, blocks in pieces:
        draws = jnp.exp(jax.random.uniform(jax.random.fold_in(own, dim), (blocks,), jnp.float32, least / len(pieces), high / len(pieces)))
        factor_of = factor_of * jnp.repeat(draws, dims[dim] // blocks).reshape([-1 if axis == dim else 1 for axis in range(len(dims))])
    return factor_of


def gaussian(rng, extent, width, most, pieces=(), held_as=jnp.bfloat16):
    entries = jax.random.normal(rng, extent, jnp.float32) * width
    if len(pieces) > 0:
        entries = block_levels(rng, extent, pieces, -0.22, 0.18) * entries
    return jnp.clip(entries, min=-most, max=most).astype(held_as)


def setup_inputs(seed: int = 0) -> dict:
    splits = jax.random.split(jax.random.key(seed), 4)
    return {
        "queries": draw_queries(jax.random.fold_in(splits[3], 71), 0),
        "keys": draw_keys(jax.random.fold_in(splits[3], 71), 0),
        "values": gaussian(splits[2], (TOKENS, KV_HEADS * HEAD_DIM), 1.0, 6.0, ((0, 8),)),
    }


def attention(queries, keys, values):
    group_size = HEADS // KV_HEADS
    score_scale = HEAD_DIM ** -0.5
    token_positions = jnp.arange(TOKENS, dtype=jnp.int32)
    allowed = token_positions[None, :] <= token_positions[:, None]

    def one_head(head_index):
        kv_index = head_index // group_size
        query_head = lax.dynamic_slice_in_dim(queries, head_index * HEAD_DIM, HEAD_DIM, 1)
        key_head = lax.dynamic_slice_in_dim(keys, kv_index * HEAD_DIM, HEAD_DIM, 1)
        value_head = lax.dynamic_slice_in_dim(values, kv_index * HEAD_DIM, HEAD_DIM, 1)
        scores = jnp.dot(query_head, key_head.T, preferred_element_type=jnp.float32) * score_scale
        scores = jnp.where(allowed, scores, -jnp.inf)
        row_peak = jnp.max(scores, axis=1, keepdims=True)
        raw_weights = jnp.where(allowed, jnp.exp(scores - row_peak), 0.0)
        row_total = jnp.sum(raw_weights, axis=1, keepdims=True)
        weights = raw_weights.astype(jnp.bfloat16)
        summed = jnp.dot(weights, value_head, preferred_element_type=jnp.float32)
        return (summed / row_total).astype(jnp.bfloat16)

    per_head = lax.map(one_head, jnp.arange(HEADS, dtype=jnp.int32))
    return jnp.transpose(per_head, (1, 0, 2)).reshape(TOKENS, HEADS * HEAD_DIM)


def reference(queries, keys, values):
    return attention(queries, keys, values)
```

```python
import functools
import math

import jax
import jax.numpy as jnp
from jax import lax
from jax.experimental import pallas as pl
from jax.experimental.pallas import tpu as pltpu
from jax.sharding import PartitionSpec as P

HEADS = 64
KV_HEADS = 8
HEAD_DIM = 128
LANES = 128
MASKED = -1e30
EXP2_SCALE = HEAD_DIM ** -0.5 * math.log2(math.e)


def attend_heads(q_v, kv, acc, peak, heads, kv_head, blocks, masked, first):
    cols = pl.ds(pl.multiple_of(kv_head * HEAD_DIM, HEAD_DIM), HEAD_DIM)
    k = jnp.concatenate([kv[b, 0, :, cols] for b in blocks], 0)
    v = jnp.concatenate([kv[b, 1, :, cols] for b in blocks], 0)
    v = jnp.concatenate([v, jnp.ones((v.shape[0], LANES), v.dtype)], 1)
    rows, count = q_v.shape[0], k.shape[0]

    def score(h):
        q = q_v[:, pl.ds(pl.multiple_of(h * HEAD_DIM, HEAD_DIM), HEAD_DIM)]
        return lax.dot_general(q, k, (((1,), (1,)), ((), ())), preferred_element_type=jnp.float32)

    def fold(h, s):
        if masked:
            row = lax.broadcasted_iota(jnp.int32, s.shape, 0)
            col = lax.broadcasted_iota(jnp.int32, s.shape, 1)
            s = jnp.where(col <= row, s, MASKED)
        top = jnp.broadcast_to(jnp.max(s, axis=1, keepdims=True), (rows, LANES))
        if not first:
            before = peak[h]
            top = jnp.maximum(before, top)
        peak[h] = top
        wide = jnp.concatenate([top] * (count // LANES), 1)
        w = jnp.exp2((s - wide) * EXP2_SCALE).astype(jnp.bfloat16)
        new = jnp.dot(w, v, preferred_element_type=jnp.float32)
        if not first:
            shrink = jnp.exp2((before - top) * EXP2_SCALE)
            new = acc[h] * jnp.concatenate([shrink, shrink], 1) + new
        acc[h] = new

    ready = score(heads[0])
    for i, h in enumerate(heads):
        upcoming = score(heads[i + 1]) if i + 1 < len(heads) else None
        fold(h, ready)
        ready = upcoming


def kernel(nc, per_dev, group, kv_dev, q_hbm, k_hbm, v_hbm, o_ref,
           q_v, kv, acc, peak, loc_sem, send_sem, fwd_sem, recv_sem):
    c = lax.axis_index("ctx")
    tp = lax.axis_index("tp")
    odd = lax.rem(c, 2)
    partner = c + 1 - 2 * odd
    shared = per_dev // kv_dev
    chunk = min(4, shared)
    first_col = pl.multiple_of(tp * per_dev // group * HEAD_DIM, HEAD_DIM)
    src = pl.ds(first_col, kv_dev * HEAD_DIM)
    load_k = pltpu.make_async_copy(k_hbm.at[:, src], kv.at[c, 0], loc_sem.at[0])
    load_v = pltpu.make_async_copy(v_hbm.at[:, src], kv.at[c, 1], loc_sem.at[1])
    load_q = pltpu.make_async_copy(q_hbm, q_v, loc_sem.at[2])
    load_k.start()
    load_v.start()
    load_q.start()

    barrier = pltpu.get_barrier_semaphore()
    pl.semaphore_signal(barrier, inc=1, device_id={"ctx": partner})
    for i in range(1, nc // 2):
        pl.semaphore_signal(barrier, inc=1, device_id={"ctx": lax.rem(c + 2 * i, nc)})
    pl.semaphore_wait(barrier, nc // 2)

    def copy_to(b, target, sem):
        return pltpu.make_async_remote_copy(
            src_ref=kv.at[b], dst_ref=kv.at[b], send_sem=sem, recv_sem=recv_sem.at[b],
            device_id={"ctx": target})

    load_k.wait()
    load_v.wait()
    sends = [(odd == 0, copy_to(c, partner, send_sem.at[0]))]
    for i in range(1, nc // 2):
        sends.append((c + 2 * i < nc, copy_to(c, lax.rem(c + 2 * i, nc), send_sem.at[i])))
    for wanted, copy in sends:
        pl.when(wanted)(copy.start)
    load_q.wait()

    def forward(p):
        mine = 2 * p + odd
        copy = copy_to(mine, partner, fwd_sem.at[p])
        copy.wait_recv()
        copy.start()

    def sweep(blocks, masked, first):
        def body(n, carry):
            heads = [n * chunk + i for i in range(chunk)]
            attend_heads(q_v, kv, acc, peak, heads, n * chunk // shared, blocks, masked, first)
            return carry
        return body

    chunks = per_dev // chunk
    pairs = c // 2
    lax.fori_loop(0, chunks, sweep([c], True, True), 0)

    @pl.when(odd == 1)
    def _():
        copy_to(c - 1, partner, send_sem.at[0]).wait_recv()
        lax.fori_loop(0, chunks, sweep([c - 1], False, False), 0)

    @pl.when(pairs > 0)
    def _():
        forward(pairs - 1)

    def pair_step(t, carry):
        p = pairs - 1 - t
        copy_to(2 * p + 1 - odd, partner, fwd_sem.at[p]).wait_recv()
        body = sweep([2 * p, 2 * p + 1], False, False)
        half = chunks // 2
        lax.fori_loop(0, half, body, 0)

        @pl.when(p > 0)
        def _():
            forward(p - 1)

        lax.fori_loop(half, chunks, body, 0)
        return carry

    lax.fori_loop(0, pairs, pair_step, 0)

    def finish(h, carry):
        out = acc[h, :, :LANES] / acc[h, :, LANES:]
        o_ref[:, pl.ds(pl.multiple_of(h * HEAD_DIM, HEAD_DIM), HEAD_DIM)] = out.astype(o_ref.dtype)
        return carry

    lax.fori_loop(0, per_dev, finish, 0)

    def drain(p, carry):
        copy_to(2 * p + odd, partner, fwd_sem.at[p]).wait_send()
        return carry

    lax.fori_loop(0, pairs, drain, 0)
    for wanted, copy in sends:
        pl.when(wanted)(copy.wait_send)


def solution(mesh):
    nc = mesh.shape["ctx"]

    def step(queries, keys, values):
        rows, width = queries.shape
        per_dev = width // HEAD_DIM
        group = HEADS // KV_HEADS
        kv_dev = per_dev // min(group, per_dev)
        any_space = pl.BlockSpec(memory_space=pltpu.HBM)
        return pl.pallas_call(
            functools.partial(kernel, nc, per_dev, group, kv_dev),
            out_shape=jax.ShapeDtypeStruct((rows, width), jnp.bfloat16),
            in_specs=[any_space] * 3,
            out_specs=pl.BlockSpec(memory_space=pltpu.VMEM),
            scratch_shapes=[
                pltpu.VMEM((rows, width), jnp.bfloat16),
                pltpu.VMEM((nc, 2, rows, kv_dev * HEAD_DIM), jnp.bfloat16),
                pltpu.VMEM((per_dev, rows, 2 * LANES), jnp.float32),
                pltpu.VMEM((per_dev, rows, LANES), jnp.float32),
                pltpu.SemaphoreType.DMA((3,)),
                pltpu.SemaphoreType.DMA((max(nc // 2, 1),)),
                pltpu.SemaphoreType.DMA((max(nc // 2, 1),)),
                pltpu.SemaphoreType.DMA((nc,)),
            ],
            compiler_params=pltpu.CompilerParams(
                collective_id=0, has_side_effects=True, vmem_limit_bytes=48 * 1024 * 1024),
        )(queries, keys, values)

    return jax.shard_map(
        step, mesh=mesh,
        in_specs=(P("ctx", "tp"), P("ctx", None), P("ctx", None)),
        out_specs=P("ctx", "tp"), check_vma=False)
```

```python
import functools
import math

import jax
import jax.numpy as jnp
from jax import lax
from jax.experimental import pallas as pl
from jax.experimental.pallas import tpu as pltpu
from jax.sharding import PartitionSpec as P

HEADS = 64
KV_HEADS = 8
HEAD_DIM = 128
LANES = 128
MASKED = -1e30
EXP2_SCALE = HEAD_DIM ** -0.5 * math.log2(math.e)


def attend_heads(q_v, kv, acc, peak, heads, kv_head, blocks, masked, first):
    k = jnp.concatenate([kv[b, kv_head, 0] for b in blocks], 0)
    v = jnp.concatenate([kv[b, kv_head, 1] for b in blocks], 0)
    v = jnp.concatenate([v, jnp.ones((v.shape[0], LANES), v.dtype)], 1)
    rows, count = q_v.shape[0], k.shape[0]

    def score(h):
        q = q_v[:, pl.ds(pl.multiple_of(h * HEAD_DIM, HEAD_DIM), HEAD_DIM)]
        return lax.dot_general(q, k, (((1,), (1,)), ((), ())), preferred_element_type=jnp.float32)

    def fold(h, s):
        if masked:
            row = lax.broadcasted_iota(jnp.int32, s.shape, 0)
            col = lax.broadcasted_iota(jnp.int32, s.shape, 1)
            s = jnp.where(col <= row, s, MASKED)
        top = jnp.broadcast_to(jnp.max(s, axis=1, keepdims=True), (rows, LANES))
        if not first:
            before = peak[h]
            top = jnp.maximum(before, top)
        peak[h] = top
        wide = jnp.concatenate([top] * (count // LANES), 1)
        w = jnp.exp2((s - wide) * EXP2_SCALE).astype(jnp.bfloat16)
        new = jnp.dot(w, v, preferred_element_type=jnp.float32)
        if not first:
            shrink = jnp.exp2((before - top) * EXP2_SCALE)
            new = acc[h] * jnp.concatenate([shrink, shrink], 1) + new
        acc[h] = new

    ready = score(heads[0])
    for i, h in enumerate(heads):
        upcoming = score(heads[i + 1]) if i + 1 < len(heads) else None
        fold(h, ready)
        ready = upcoming


def kernel(nc, per_dev, group, kv_dev, q_hbm, k_hbm, v_hbm, o_ref,
           q_v, kv, acc, peak, loc_sem, send_sem, fwd_sem, far_sem, recv_sem):
    c = lax.axis_index("ctx")
    tp = lax.axis_index("tp")
    odd = lax.rem(c, 2)
    pair = c // 2
    partner = c + 1 - 2 * odd
    shared = per_dev // kv_dev
    chunk = min(4, shared)
    square = nc == 8 and kv_dev == 2
    base = tp * per_dev // group

    loads = []
    for g in range(kv_dev):
        cols = pl.ds(pl.multiple_of((base + g) * HEAD_DIM, HEAD_DIM), HEAD_DIM)
        loads.append([
            pltpu.make_async_copy(ref.at[:, cols], kv.at[c, g, i], loc_sem.at[2 * g + i])
            for i, ref in enumerate((k_hbm, v_hbm))])
        for load in loads[g]:
            load.start()
    load_q = pltpu.make_async_copy(q_hbm, q_v, loc_sem.at[2 * kv_dev])
    load_q.start()

    barrier = pltpu.get_barrier_semaphore()
    pl.semaphore_signal(barrier, inc=1, device_id={"ctx": partner})
    for i in range(1, nc // 2):
        pl.semaphore_signal(barrier, inc=1, device_id={"ctx": lax.rem(c + 2 * i, nc)})
    pl.semaphore_wait(barrier, nc // 2)

    def copy_to(b, g, target, sem):
        return pltpu.make_async_remote_copy(
            src_ref=kv.at[b, g], dst_ref=kv.at[b, g], send_sem=sem, recv_sem=recv_sem.at[b, g],
            device_id={"ctx": target})

    for load in sum(loads, []):
        load.wait()
    sends = []
    for g in range(kv_dev):
        sends.append((odd == 0, copy_to(c, g, partner, send_sem.at[0, g])))
        if square:
            sends.append((lax.rem(pair, 2) == 0, copy_to(c, g, lax.rem(c + 2, nc), send_sem.at[1, g])))
            first = kv_dev - 1 - g
            other = lax.select(pair == 0, first, g)
            sends.append((pair < 2, copy_to(c, other, lax.rem(c + 4, nc), send_sem.at[2, g])))
        else:
            for i in range(1, nc // 2):
                sends.append((c + 2 * i < nc, copy_to(c, g, lax.rem(c + 2 * i, nc), send_sem.at[i, g])))
    for wanted, copy in sends:
        pl.when(wanted)(copy.start)
    load_q.wait()

    def item(t):
        if not square:
            return pair - 1 - t // kv_dev, lax.rem(t, kv_dev)
        third = (lax.select(t < 4, 2 - lax.rem(t, 2), 0), lax.select(t < 4, t // 2, t - 4))
        second = (t // 2, lax.rem((t + 1) // 2 + 1, 2))
        return (lax.select(pair == 3, third[0], lax.select(pair == 2, second[0], 0)),
                lax.select(pair == 3, third[1], lax.select(pair == 2, second[1], t)))

    def onward(p, g):
        mine = 2 * p + odd
        up = ((pair == 1) & (g == 0)) | ((pair == 2) & (p == 0) & (g == 1))
        back = (pair == 3) & (p == 1)
        target = lax.select(pair == 3, 4 + odd, 6 + odd)
        return up | back, copy_to(mine, g, target, far_sem.at[p, g])

    def pull(t):
        p, g = item(t)
        copy = copy_to(2 * p + odd, g, partner, fwd_sem.at[p, g])
        copy.wait_recv()
        if square:
            wanted, far = onward(p, g)
            pl.when(wanted)(far.start)
        copy.start()

    def sweep(blocks, kv_head, masked, first):
        def body(n, carry):
            heads = [n * chunk + i for i in range(chunk)]
            g = n * chunk // shared if kv_head is None else kv_head
            attend_heads(q_v, kv, acc, peak, heads, g, blocks, masked, first)
            return carry
        return body

    def finish(h, carry):
        out = acc[h, :, :LANES] / acc[h, :, LANES:]
        o_ref[:, pl.ds(pl.multiple_of(h * HEAD_DIM, HEAD_DIM), HEAD_DIM)] = out.astype(o_ref.dtype)
        return carry

    chunks = per_dev // chunk
    steps = pair * kv_dev
    lax.fori_loop(0, chunks, sweep([c], None, True, True), 0)

    @pl.when(odd == 1)
    def _():
        for g in range(kv_dev):
            copy_to(c - 1, g, partner, send_sem.at[0, g]).wait_recv()
        lax.fori_loop(0, chunks, sweep([c - 1], None, False, False), 0)

    @pl.when(pair > 0)
    def _():
        pull(0)

    def step(t, carry):
        p, g = item(t)
        copy_to(2 * p + 1 - odd, g, partner, fwd_sem.at[p, g]).wait_recv()
        body = sweep([2 * p, 2 * p + 1], g, False, False)
        per_head = shared // chunk
        start = g * per_head
        half = start + per_head // 2
        lax.fori_loop(start, half, body, 0)

        @pl.when(t + 1 < steps)
        def _():
            pull(t + 1)

        lax.fori_loop(half, start + per_head, body, 0)

        @pl.when(t >= steps - kv_dev)
        def _():
            lax.fori_loop(g * shared, (g + 1) * shared, finish, 0)
        return carry

    lax.fori_loop(0, steps, step, 0)

    @pl.when(pair == 0)
    def _():
        lax.fori_loop(0, per_dev, finish, 0)

    def drain(t, carry):
        p, g = item(t)
        copy_to(2 * p + odd, g, partner, fwd_sem.at[p, g]).wait_send()
        if square:
            wanted, far = onward(p, g)
            pl.when(wanted)(far.wait_send)
        return carry

    lax.fori_loop(0, steps, drain, 0)
    for wanted, copy in sends:
        pl.when(wanted)(copy.wait_send)


def solution(mesh):
    nc = mesh.shape["ctx"]

    def step(queries, keys, values):
        rows, width = queries.shape
        per_dev = width // HEAD_DIM
        group = HEADS // KV_HEADS
        kv_dev = per_dev // min(group, per_dev)
        any_space = pl.BlockSpec(memory_space=pltpu.HBM)
        return pl.pallas_call(
            functools.partial(kernel, nc, per_dev, group, kv_dev),
            out_shape=jax.ShapeDtypeStruct((rows, width), jnp.bfloat16),
            in_specs=[any_space] * 3,
            out_specs=pl.BlockSpec(memory_space=pltpu.VMEM),
            scratch_shapes=[
                pltpu.VMEM((rows, width), jnp.bfloat16),
                pltpu.VMEM((nc, kv_dev, 2, rows, HEAD_DIM), jnp.bfloat16),
                pltpu.VMEM((per_dev, rows, 2 * LANES), jnp.float32),
                pltpu.VMEM((per_dev, rows, LANES), jnp.float32),
                pltpu.SemaphoreType.DMA((2 * kv_dev + 1,)),
                pltpu.SemaphoreType.DMA((nc // 2, kv_dev)),
                pltpu.SemaphoreType.DMA((nc // 2, kv_dev)),
                pltpu.SemaphoreType.DMA((nc // 2, kv_dev)),
                pltpu.SemaphoreType.DMA((nc, kv_dev)),
            ],
            compiler_params=pltpu.CompilerParams(
                collective_id=0, has_side_effects=True, vmem_limit_bytes=60 * 1024 * 1024),
        )(queries, keys, values)

    return jax.shard_map(
        step, mesh=mesh,
        in_specs=(P("ctx", "tp"), P("ctx", None), P("ctx", None)),
        out_specs=P("ctx", "tp"), check_vma=False)
```

```python
import functools
import math

import jax
import jax.numpy as jnp
from jax import lax
from jax.experimental import pallas as pl
from jax.experimental.pallas import tpu as pltpu
from jax.sharding import PartitionSpec as P

HEADS = 64
KV_HEADS = 8
HEAD_DIM = 128
LANES = 128
MASKED = -1e30
CHUNK = 8
DEPTH = 1
ROUTED = 1
EXP2_SCALE = HEAD_DIM ** -0.5 * math.log2(math.e)


def attend_heads(q_v, kv, acc, peak, heads, kv_head, blocks, masked, first):
    k = jnp.concatenate([kv[b, kv_head, 0] for b in blocks], 0)
    v = jnp.concatenate([kv[b, kv_head, 1] for b in blocks], 0)
    v = jnp.concatenate([v, jnp.ones((v.shape[0], LANES), v.dtype)], 1)
    rows, count = q_v.shape[0], k.shape[0]

    def score(h):
        q = q_v[:, pl.ds(pl.multiple_of(h * HEAD_DIM, HEAD_DIM), HEAD_DIM)]
        return lax.dot_general(q, k, (((1,), (1,)), ((), ())), preferred_element_type=jnp.float32)

    def fold(h, s):
        if masked:
            row = lax.broadcasted_iota(jnp.int32, s.shape, 0)
            col = lax.broadcasted_iota(jnp.int32, s.shape, 1)
            s = jnp.where(col <= row, s, MASKED)
        top = jnp.broadcast_to(jnp.max(s, axis=1, keepdims=True), (rows, LANES))
        if not first:
            before = peak[h]
            top = jnp.maximum(before, top)
        peak[h] = top
        wide = jnp.concatenate([top] * (count // LANES), 1)
        w = jnp.exp2((s - wide) * EXP2_SCALE).astype(jnp.bfloat16)
        new = jnp.dot(w, v, preferred_element_type=jnp.float32)
        if not first:
            shrink = jnp.exp2((before - top) * EXP2_SCALE)
            new = acc[h] * jnp.concatenate([shrink, shrink], 1) + new
        acc[h] = new

    ahead = [score(h) for h in heads[:DEPTH]]
    for i, h in enumerate(heads):
        if i + DEPTH < len(heads):
            ahead.append(score(heads[i + DEPTH]))
        fold(h, ahead.pop(0))


def kernel(nc, per_dev, group, kv_dev, q_hbm, k_hbm, v_hbm, o_ref,
           q_v, kv, acc, peak, loc_sem, send_sem, fwd_sem, far_sem, recv_sem):
    c = lax.axis_index("ctx")
    tp = lax.axis_index("tp")
    odd = lax.rem(c, 2)
    pair = c // 2
    partner = c + 1 - 2 * odd
    shared = per_dev // kv_dev
    chunk = min(CHUNK, shared)
    square = nc == 8 and kv_dev == 2
    base = tp * per_dev // group

    loads = []
    for g in range(kv_dev):
        cols = pl.ds(pl.multiple_of((base + g) * HEAD_DIM, HEAD_DIM), HEAD_DIM)
        loads.append([
            pltpu.make_async_copy(ref.at[:, cols], kv.at[c, g, i], loc_sem.at[2 * g + i])
            for i, ref in enumerate((k_hbm, v_hbm))])
        for load in loads[g]:
            load.start()
    load_q = pltpu.make_async_copy(q_hbm, q_v, loc_sem.at[2 * kv_dev])
    load_q.start()

    barrier = pltpu.get_barrier_semaphore()
    pl.semaphore_signal(barrier, inc=1, device_id={"ctx": partner})
    for i in range(1, nc // 2):
        pl.semaphore_signal(barrier, inc=1, device_id={"ctx": lax.rem(c + 2 * i, nc)})
    pl.semaphore_wait(barrier, nc // 2)

    def copy_to(b, g, target, sem):
        return pltpu.make_async_remote_copy(
            src_ref=kv.at[b, g], dst_ref=kv.at[b, g], send_sem=sem, recv_sem=recv_sem.at[b, g],
            device_id={"ctx": target})

    for load in sum(loads, []):
        load.wait()
    sends = []
    for g in range(kv_dev):
        sends.append((odd == 0, copy_to(c, g, partner, send_sem.at[0, g])))
        if square:
            beside = (lax.rem(pair, 2) == 0) if g < ROUTED else (pair < 3)
            sends.append((beside, copy_to(c, g, lax.rem(c + 2, nc), send_sem.at[1, g])))
            first = kv_dev - 1 - g
            other = lax.select(pair == 0, first, g)
            sends.append((pair < 2, copy_to(c, other, lax.rem(c + 4, nc), send_sem.at[2, g])))
        else:
            for i in range(1, nc // 2):
                sends.append((c + 2 * i < nc, copy_to(c, g, lax.rem(c + 2 * i, nc), send_sem.at[i, g])))
    for wanted, copy in sends:
        pl.when(wanted)(copy.start)
    load_q.wait()

    def item(t):
        if not square:
            return pair - 1 - t // kv_dev, lax.rem(t, kv_dev)
        third = (lax.select(t < 4, 2 - lax.rem(t, 2), 0), lax.select(t < 4, t // 2, t - 4))
        second = (t // 2, lax.rem((t + 1) // 2 + 1, 2))
        return (lax.select(pair == 3, third[0], lax.select(pair == 2, second[0], 0)),
                lax.select(pair == 3, third[1], lax.select(pair == 2, second[1], t)))

    def onward(p, g):
        mine = 2 * p + odd
        up = ((pair == 1) & (g == 0)) | ((pair == 2) & (p == 0) & (g == 1))
        back = (pair == 3) & (p == 1) & (g < ROUTED)
        target = lax.select(pair == 3, 4 + odd, 6 + odd)
        return up | back, copy_to(mine, g, target, far_sem.at[p, g])

    def pull(t):
        p, g = item(t)
        copy = copy_to(2 * p + odd, g, partner, fwd_sem.at[p, g])
        copy.wait_recv()
        if square:
            wanted, far = onward(p, g)
            pl.when(wanted)(far.start)
        copy.start()

    def sweep(blocks, kv_head, masked, first):
        def body(n, carry):
            heads = [n * chunk + i for i in range(chunk)]
            g = n * chunk // shared if kv_head is None else kv_head
            attend_heads(q_v, kv, acc, peak, heads, g, blocks, masked, first)
            return carry
        return body

    def finish(h, carry):
        out = acc[h, :, :LANES] / acc[h, :, LANES:]
        o_ref[:, pl.ds(pl.multiple_of(h * HEAD_DIM, HEAD_DIM), HEAD_DIM)] = out.astype(o_ref.dtype)
        return carry

    chunks = per_dev // chunk
    steps = pair * kv_dev
    lax.fori_loop(0, chunks, sweep([c], None, True, True), 0)

    @pl.when(odd == 1)
    def _():
        for g in range(kv_dev):
            copy_to(c - 1, g, partner, send_sem.at[0, g]).wait_recv()
        lax.fori_loop(0, chunks, sweep([c - 1], None, False, False), 0)

    @pl.when(pair > 0)
    def _():
        pull(0)

    def step(t, carry):
        p, g = item(t)
        copy_to(2 * p + 1 - odd, g, partner, fwd_sem.at[p, g]).wait_recv()
        body = sweep([2 * p, 2 * p + 1], g, False, False)

        @pl.when(t + 1 < steps)
        def _():
            pull(t + 1)

        per_head = shared // chunk
        lax.fori_loop(g * per_head, (g + 1) * per_head, body, 0)

        @pl.when(t >= steps - kv_dev)
        def _():
            lax.fori_loop(g * shared, (g + 1) * shared, finish, 0)
        return carry

    lax.fori_loop(0, steps, step, 0)

    @pl.when(pair == 0)
    def _():
        lax.fori_loop(0, per_dev, finish, 0)

    def drain(t, carry):
        p, g = item(t)
        copy_to(2 * p + odd, g, partner, fwd_sem.at[p, g]).wait_send()
        if square:
            wanted, far = onward(p, g)
            pl.when(wanted)(far.wait_send)
        return carry

    lax.fori_loop(0, steps, drain, 0)
    for wanted, copy in sends:
        pl.when(wanted)(copy.wait_send)


def solution(mesh):
    nc = mesh.shape["ctx"]

    def step(queries, keys, values):
        rows, width = queries.shape
        per_dev = width // HEAD_DIM
        group = HEADS // KV_HEADS
        kv_dev = per_dev // min(group, per_dev)
        any_space = pl.BlockSpec(memory_space=pltpu.HBM)
        return pl.pallas_call(
            functools.partial(kernel, nc, per_dev, group, kv_dev),
            out_shape=pltpu.VMEM((rows, width), jnp.bfloat16),
            in_specs=[any_space] * 3,
            out_specs=pl.BlockSpec(memory_space=pltpu.VMEM),
            scratch_shapes=[
                pltpu.VMEM((rows, width), jnp.bfloat16),
                pltpu.VMEM((nc, kv_dev, 2, rows, HEAD_DIM), jnp.bfloat16),
                pltpu.VMEM((per_dev, rows, 2 * LANES), jnp.float32),
                pltpu.VMEM((per_dev, rows, LANES), jnp.float32),
                pltpu.SemaphoreType.DMA((2 * kv_dev + 1,)),
                pltpu.SemaphoreType.DMA((nc // 2, kv_dev)),
                pltpu.SemaphoreType.DMA((nc // 2, kv_dev)),
                pltpu.SemaphoreType.DMA((nc // 2, kv_dev)),
                pltpu.SemaphoreType.DMA((nc, kv_dev)),
            ],
            compiler_params=pltpu.CompilerParams(
                collective_id=0, has_side_effects=True, vmem_limit_bytes=60 * 1024 * 1024),
        )(queries, keys, values)

    return jax.shard_map(
        step, mesh=mesh,
        in_specs=(P("ctx", "tp"), P("ctx", None), P("ctx", None)),
        out_specs=P("ctx", "tp"), check_vma=False)
```
